32 devices in a mesh: vp: 4 (over z), dp: 8 (over y, x, core).
Axes of the slice: x: 2, y: 2, z: 4, core: 2. Of those that a mesh axis runs over, the one named last changes fastest.
Arguments:
- student_x: bfloat16 [5120, 384], P('dp')
- teacher_x: bfloat16 [1024, 384], P('dp')
- w_in: bfloat16 [384, 2048], replicated
- b_in: bfloat16 [2048], replicated
- w_mid: bfloat16 [2048, 2048], replicated
- b_mid: bfloat16 [2048], replicated
- w_out: bfloat16 [2048, 256], replicated
- b_out: bfloat16 [256], replicated
- protos: bfloat16 [256, 65536], P(None, 'vp')
- ema_w_in: bfloat16 [384, 2048], replicated
- ema_b_in: bfloat16 [2048], replicated
- ema_w_mid: bfloat16 [2048, 2048], replicated
- ema_b_mid: bfloat16 [2048], replicated
- ema_w_out: bfloat16 [2048, 256], replicated
- ema_b_out: bfloat16 [256], replicated
- ema_protos: bfloat16 [256, 65536], P(None, 'vp')
Outputs:
- output 1: float32 [], replicated
- output 2: float32 [384, 2048], replicated
- output 3: float32 [2048], replicated
- output 4: float32 [2048, 2048], replicated
- output 5: float32 [2048], replicated
- output 6: float32 [2048, 256], replicated
- output 7: float32 [256], replicated
- output 8: float32 [256, 65536], P(None, 'vp')
All inputs are finite; a program needn't handle non-finite values.
Results may differ from the reference program's by a relative error of at most 0.00519324.
Values sent between devices are 32-bit elements.
A program may use at most 1 GiB of HBM per device.

```python
import jax
import jax.numpy as jnp
from jax import lax
from functools import partial

EMBED_DIM = 384
HIDDEN_DIM = 2048
BOTTLENECK = 256
PROTOTYPES = 65536
TOTAL_IMAGES = 512
ALL_CROPS = 10
GLOBAL_CROPS = 2
SINK_ITERS = 3
IMAGE_BLOCK = 8
TEMP_STUDENT = 0.1
TEMP_TEACHER = 0.04


def setup_inputs(seed: int = 0) -> dict:
    keys = jax.random.split(jax.random.key(seed), 20)
    n_clusters = 4
    centers = jax.random.normal(keys[0], (n_clusters, EMBED_DIM), jnp.float32)
    cluster_of = (jnp.arange(TOTAL_IMAGES) * n_clusters) // TOTAL_IMAGES
    img_mean = centers[cluster_of] + 0.7 * jax.random.normal(keys[1], (TOTAL_IMAGES, EMBED_DIM), jnp.float32)
    teacher_x = img_mean[:, None, :] + 0.5 * jax.random.normal(keys[2], (TOTAL_IMAGES, GLOBAL_CROPS, EMBED_DIM), jnp.float32)
    student_x = img_mean[:, None, :] + 0.7 * jax.random.normal(keys[3], (TOTAL_IMAGES, ALL_CROPS, EMBED_DIM), jnp.float32)

    def make_dense(key, fan_in, fan_out):
        return jax.random.normal(key, (fan_in, fan_out), jnp.float32) * fan_in ** -0.5

    def make_bias(key, width):
        return 0.5 * jax.random.normal(key, (width,), jnp.float32)

    w_in = make_dense(keys[4], EMBED_DIM, HIDDEN_DIM)
    b_in = make_bias(keys[5], HIDDEN_DIM)
    w_mid = make_dense(keys[6], HIDDEN_DIM, HIDDEN_DIM)
    b_mid = make_bias(keys[7], HIDDEN_DIM)
    w_out = make_dense(keys[8], HIDDEN_DIM, BOTTLENECK)
    b_out = make_bias(keys[9], BOTTLENECK)
    col_scale = jnp.exp(0.5 * jax.random.normal(keys[10], (1, PROTOTYPES), jnp.float32))
    protos = jax.random.normal(keys[11], (BOTTLENECK, PROTOTYPES), jnp.float32) * col_scale
    ema_w_in = 0.8 * w_in + 0.6 * make_dense(keys[12], EMBED_DIM, HIDDEN_DIM)
    ema_b_in = 0.8 * b_in + 0.6 * make_bias(keys[13], HIDDEN_DIM)
    ema_w_mid = 0.8 * w_mid + 0.6 * make_dense(keys[14], HIDDEN_DIM, HIDDEN_DIM)
    ema_b_mid = 0.8 * b_mid + 0.6 * make_bias(keys[15], HIDDEN_DIM)
    ema_w_out = 0.8 * w_out + 0.6 * make_dense(keys[16], HIDDEN_DIM, BOTTLENECK)
    ema_b_out = 0.8 * b_out + 0.6 * make_bias(keys[17], BOTTLENECK)
    ema_protos = 0.8 * protos + 0.6 * jax.random.normal(keys[18], (BOTTLENECK, PROTOTYPES), jnp.float32) * col_scale
    return {
        'student_x': student_x.reshape(TOTAL_IMAGES * ALL_CROPS, EMBED_DIM).astype(jnp.bfloat16),
        'teacher_x': teacher_x.reshape(TOTAL_IMAGES * GLOBAL_CROPS, EMBED_DIM).astype(jnp.bfloat16),
        'w_in': w_in.astype(jnp.bfloat16),
        'b_in': b_in.astype(jnp.bfloat16),
        'w_mid': w_mid.astype(jnp.bfloat16),
        'b_mid': b_mid.astype(jnp.bfloat16),
        'w_out': w_out.astype(jnp.bfloat16),
        'b_out': b_out.astype(jnp.bfloat16),
        'protos': protos.astype(jnp.bfloat16),
        'ema_w_in': ema_w_in.astype(jnp.bfloat16),
        'ema_b_in': ema_b_in.astype(jnp.bfloat16),
        'ema_w_mid': ema_w_mid.astype(jnp.bfloat16),
        'ema_b_mid': ema_b_mid.astype(jnp.bfloat16),
        'ema_w_out': ema_w_out.astype(jnp.bfloat16),
        'ema_b_out': ema_b_out.astype(jnp.bfloat16),
        'ema_protos': ema_protos.astype(jnp.bfloat16),
    }


def snap_bf16(vals):
    return vals.astype(jnp.bfloat16).astype(jnp.float32)


def head_mlp(feats, w_in, b_in, w_mid, b_mid, w_out, b_out):
    hid_one = snap_bf16(jax.nn.gelu(jnp.dot(feats, w_in, preferred_element_type=jnp.float32) + b_in, approximate=False))
    hid_two = snap_bf16(jax.nn.gelu(jnp.dot(hid_one, w_mid, preferred_element_type=jnp.float32) + b_mid, approximate=False))
    proj = jnp.dot(hid_two, w_out, preferred_element_type=jnp.float32) + b_out
    return snap_bf16(proj / jnp.sqrt(jnp.sum(proj * proj, axis=-1, keepdims=True)))


def col_normalize(protos):
    return snap_bf16(protos / jnp.sqrt(jnp.sum(protos * protos, axis=0, keepdims=True)))


def block_loss(q_blk, emb_blk, proto_mat):
    logits = jnp.dot(emb_blk, proto_mat, preferred_element_type=jnp.float32) / TEMP_STUDENT
    log_p = jax.nn.log_softmax(logits.reshape(IMAGE_BLOCK, ALL_CROPS, PROTOTYPES), axis=-1)
    cross = jnp.einsum('iak,ivk->iav', q_blk, log_p)
    pair_mask = (jnp.arange(GLOBAL_CROPS)[:, None] != jnp.arange(ALL_CROPS)[None, :]).astype(jnp.float32)
    return -jnp.sum(cross * pair_mask) / (TOTAL_IMAGES * GLOBAL_CROPS * (ALL_CROPS - 1))


def reference(student_x, teacher_x, w_in, b_in, w_mid, b_mid, w_out, b_out, protos,
              ema_w_in, ema_b_in, ema_w_mid, ema_b_mid, ema_w_out, ema_b_out, ema_protos):
    t_emb = head_mlp(teacher_x.astype(jnp.float32), ema_w_in.astype(jnp.float32), ema_b_in.astype(jnp.float32),
                     ema_w_mid.astype(jnp.float32), ema_b_mid.astype(jnp.float32),
                     ema_w_out.astype(jnp.float32), ema_b_out.astype(jnp.float32))
    t_logits = jnp.dot(t_emb, col_normalize(ema_protos.astype(jnp.float32)), preferred_element_type=jnp.float32)
    n_rows = GLOBAL_CROPS * TOTAL_IMAGES
    q_mat = jnp.exp(t_logits / TEMP_TEACHER)
    q_mat = q_mat / jnp.sum(q_mat)
    for _ in range(SINK_ITERS):
        q_mat = q_mat / jnp.sum(q_mat, axis=0, keepdims=True) / PROTOTYPES
        q_mat = q_mat / jnp.sum(q_mat, axis=1, keepdims=True) / n_rows
    q_mat = q_mat * n_rows
    n_blocks = TOTAL_IMAGES // IMAGE_BLOCK
    q_blocks = q_mat.reshape(n_blocks, IMAGE_BLOCK, GLOBAL_CROPS, PROTOTYPES)

    feats = student_x.astype(jnp.float32)
    student_params = (w_in.astype(jnp.float32), b_in.astype(jnp.float32), w_mid.astype(jnp.float32),
                      b_mid.astype(jnp.float32), w_out.astype(jnp.float32), b_out.astype(jnp.float32))

    def student_embed(params):
        return head_mlp(feats, params[0], params[1], params[2], params[3], params[4], params[5])

    s_emb, emb_vjp = jax.vjp(student_embed, student_params)
    proto_unit, proto_vjp = jax.vjp(col_normalize, protos.astype(jnp.float32))
    emb_blocks = s_emb.reshape(n_blocks, IMAGE_BLOCK * ALL_CROPS, BOTTLENECK)

    def scan_step(carry, blk):
        q_blk, emb_blk = blk
        part_loss, blk_vjp = jax.vjp(partial(block_loss, q_blk), emb_blk, proto_unit)
        g_emb_blk, g_unit_blk = blk_vjp(jnp.ones((), jnp.float32))
        return (carry[0] + part_loss, carry[1] + g_unit_blk), g_emb_blk

    init = (jnp.zeros((), jnp.float32), jnp.zeros((BOTTLENECK, PROTOTYPES), jnp.float32))
    (loss, g_unit), g_emb = lax.scan(scan_step, init, (q_blocks, emb_blocks))
    g_params = emb_vjp(g_emb.reshape(TOTAL_IMAGES * ALL_CROPS, BOTTLENECK))[0]
    g_protos = proto_vjp(g_unit)[0]
    return (loss, g_params[0], g_params[1], g_params[2], g_params[3], g_params[4], g_params[5], g_protos)
```

```python
import jax
import jax.numpy as jnp
from jax import lax
from jax.sharding import PartitionSpec as P

ALL_CROPS = 10
GLOBAL_CROPS = 2
SINK_ITERS = 3
TEMP_STUDENT = 0.1
TEMP_TEACHER = 0.04
F32 = jnp.float32
BF16 = jnp.bfloat16


def gelu_slope(pre):
    cdf = 0.5 * (1.0 + lax.erf(pre * 0.7071067811865476))
    return cdf + pre * jnp.exp(-0.5 * pre * pre) * 0.3989422804014327


def mlp_forward(feats, w_in, b_in, w_mid, b_mid, w_out, b_out):
    pre_one = jnp.dot(feats, w_in, preferred_element_type=F32) + b_in.astype(F32)
    hid_one = jax.nn.gelu(pre_one, approximate=False).astype(BF16)
    pre_two = jnp.dot(hid_one, w_mid, preferred_element_type=F32) + b_mid.astype(F32)
    hid_two = jax.nn.gelu(pre_two, approximate=False).astype(BF16)
    proj = jnp.dot(hid_two, w_out, preferred_element_type=F32) + b_out.astype(F32)
    inv_norm = lax.rsqrt(jnp.sum(proj * proj, axis=-1, keepdims=True))
    unit = proj * inv_norm
    return unit.astype(BF16), proj, (pre_one, hid_one, pre_two, hid_two, unit, inv_norm)


def col_normalize(protos):
    proto_f = protos.astype(F32)
    inv_col = lax.rsqrt(jnp.sum(proto_f * proto_f, axis=0, keepdims=True))
    unit = proto_f * inv_col
    return unit.astype(BF16), unit, inv_col


def pair_targets(q_three):
    pad_rows = ALL_CROPS - GLOBAL_CROPS
    return jnp.sum(q_three, axis=1, keepdims=True) - jnp.pad(q_three, ((0, 0), (0, pad_rows), (0, 0)))


def crop_counts():
    crop_idx = jnp.arange(ALL_CROPS)
    return (GLOBAL_CROPS - (crop_idx < GLOBAL_CROPS).astype(jnp.int32)).astype(F32)


def solution(mesh):
    vp_size = mesh.shape['vp']
    dp_size = mesh.shape['dp']

    def local_step(student_x, teacher_x, w_in, b_in, w_mid, b_mid, w_out, b_out, protos,
                   ema_w_in, ema_b_in, ema_w_mid, ema_b_mid, ema_w_out, ema_b_out, ema_protos):
        n_img = student_x.shape[0] // ALL_CROPS
        local_proto = protos.shape[1]
        n_proto = local_proto * vp_size
        n_rows = GLOBAL_CROPS * n_img * dp_size
        hidden = w_mid.shape[0]
        bott = w_out.shape[1]
        in_dim = w_in.shape[0]
        i_dp = lax.axis_index('dp')
        i_vp = lax.axis_index('vp')
        scale = 1.0 / (n_img * dp_size * GLOBAL_CROPS * (ALL_CROPS - 1))

        t_emb, t_proj, _ = mlp_forward(teacher_x, ema_w_in, ema_b_in, ema_w_mid, ema_b_mid, ema_w_out, ema_b_out)
        t_unit = col_normalize(ema_protos)[0]
        e_mat = jnp.exp(jnp.dot(t_emb, t_unit, preferred_element_type=F32) / TEMP_TEACHER)
        col_raw = lax.psum(jnp.sum(e_mat, axis=0, keepdims=True), 'dp')

        s_emb, s_proj, saved = mlp_forward(student_x, w_in, b_in, w_mid, b_mid, w_out, b_out)
        s_unit = col_normalize(protos)[0]
        emb_all = lax.all_gather(jnp.concatenate([s_proj, t_proj], axis=0), 'dp', axis=0)
        emb_all = emb_all * lax.rsqrt(jnp.sum(emb_all * emb_all, axis=-1, keepdims=True))
        logits = jnp.dot(s_emb, s_unit, preferred_element_type=F32) / TEMP_STUDENT
        exp_s = jnp.exp(logits)
        srow = jnp.sum(exp_s, axis=-1, keepdims=True)

        b_raw = 1.0 / (col_raw * n_proto)
        rows = jnp.sum(e_mat * b_raw, axis=1, keepdims=True)
        tot = jnp.sum(col_raw).reshape(1, 1)
        packed = lax.psum(jnp.concatenate([rows, srow, tot], axis=0), 'vp')
        nt = rows.shape[0]
        total = packed[-1:, :]
        row_sum = packed[nt:-1, :]
        inv_total = 1.0 / total
        a_vec = inv_total / ((packed[:nt, :] * (inv_total * total)) * n_rows)
        b_vec = b_raw * total
        for _ in range(SINK_ITERS - 1):
            col = lax.psum(jnp.sum(e_mat * a_vec, axis=0, keepdims=True), 'dp')
            b_vec = 1.0 / (col * n_proto)
            row = lax.psum(jnp.sum(e_mat * b_vec, axis=1, keepdims=True), 'vp')
            a_vec = 1.0 / (row * n_rows)
        a_fin = a_vec * n_rows

        def grad_logits(logit, e_blk, a_col, b_row, rsum):
            nr = logit.shape[0]
            kk = logit.shape[1]
            q_three = (e_blk * a_col * b_row).reshape(nr // ALL_CROPS, GLOBAL_CROPS, kk)
            targets = pair_targets(q_three)
            prob = (jnp.exp(logit) / rsum).reshape(nr // ALL_CROPS, ALL_CROPS, kk)
            g = (crop_counts()[:, None] * prob - targets) * (scale / TEMP_STUDENT)
            return g.reshape(nr, kk).astype(BF16), targets

        g_logits, targets = grad_logits(logits, e_mat, a_fin, b_vec, row_sum)
        lg3 = logits.reshape(targets.shape)
        loss_part = jnp.sum(targets * (jnp.log(row_sum).reshape(n_img, ALL_CROPS, 1) - lg3)) * scale
        g_emb = lax.psum(jnp.einsum('rk,bk->rb', g_logits, s_unit, preferred_element_type=F32), 'vp')

        own = local_proto // dp_size
        c0 = i_dp * own
        small = lax.all_gather(jnp.concatenate([row_sum, a_fin], axis=0), 'dp', axis=0)
        n_s = s_emb.shape[0]
        s_all = emb_all[:, :n_s].reshape(-1, bott).astype(BF16)
        t_all = emb_all[:, n_s:].reshape(-1, bott).astype(BF16)
        rs_all = small[:, :n_s].reshape(-1, 1)
        a_all = small[:, n_s:].reshape(-1, 1)
        p_own = lax.dynamic_slice_in_dim(protos, c0, own, axis=1)
        su_own, su_f, inv_own = col_normalize(p_own)
        tu_own = col_normalize(lax.dynamic_slice_in_dim(ema_protos, c0, own, axis=1))[0]
        b_own = lax.dynamic_slice_in_dim(b_vec, c0, own, axis=1)
        lg_own = jnp.dot(s_all, su_own, preferred_element_type=F32) / TEMP_STUDENT
        e_own = jnp.exp(jnp.dot(t_all, tu_own, preferred_element_type=F32) / TEMP_TEACHER)
        gl_own, _ = grad_logits(lg_own, e_own, a_all, b_own, rs_all)
        gu = jnp.einsum('rb,rk->bk', s_all, gl_own, preferred_element_type=F32)
        gp_own = (gu - su_f * jnp.sum(su_f * gu, axis=0, keepdims=True)) * inv_own
        g_protos = lax.all_gather(gp_own, 'dp', axis=1, tiled=True)

        pre_one, hid_one, pre_two, hid_two, unit, inv_norm = saved
        qh = hidden // vp_size
        h0 = i_vp * qh
        g_proj = (g_emb - unit * jnp.sum(unit * g_emb, axis=-1, keepdims=True)) * inv_norm
        g_proj_lo = g_proj.astype(BF16)
        g_hid_two = jnp.einsum('nb,hb->nh', g_proj_lo, w_out, preferred_element_type=F32)
        g_pre_two = g_hid_two * gelu_slope(pre_two)
        g_pre_two_lo = g_pre_two.astype(BF16)
        hid_two_q = lax.dynamic_slice_in_dim(hid_two, h0, qh, axis=1)
        hid_one_q = lax.dynamic_slice_in_dim(hid_one, h0, qh, axis=1)
        pre_one_q = lax.dynamic_slice_in_dim(pre_one, h0, qh, axis=1)
        w_mid_q = lax.dynamic_slice_in_dim(w_mid, h0, qh, axis=0)
        g_w_out_q = jnp.einsum('nh,nb->hb', hid_two_q, g_proj_lo, preferred_element_type=F32)
        g_w_mid_q = jnp.einsum('ng,nh->gh', hid_one_q, g_pre_two_lo, preferred_element_type=F32)
        g_hid_one_q = jnp.einsum('nh,gh->ng', g_pre_two_lo, w_mid_q, preferred_element_type=F32)
        g_pre_one_q = g_hid_one_q * gelu_slope(pre_one_q)
        g_w_in_q = jnp.einsum('nh,nf->hf', g_pre_one_q.astype(BF16), student_x, preferred_element_type=F32)
        bq = bott // vp_size
        gb_in = jnp.sum(g_pre_one_q, axis=0)
        gb_mid = lax.dynamic_slice_in_dim(jnp.sum(g_pre_two, axis=0), h0, qh, axis=0)
        gb_out = lax.dynamic_slice_in_dim(jnp.sum(g_proj, axis=0), i_vp * bq, bq, axis=0)
        tail = jnp.stack([gb_in, gb_mid, jnp.pad(gb_out, (0, qh - bq)),
                          jnp.pad(loss_part.reshape(1), (0, qh - 1))], axis=1)
        stack = jnp.concatenate([g_w_mid_q, g_w_in_q, g_w_out_q, jnp.pad(tail, ((0, 0), (0, 124)))], axis=1)
        part = lax.psum_scatter(stack, 'dp', scatter_dimension=0, tiled=True)
        full = lax.all_gather(part, ('vp', 'dp'), axis=0, tiled=True)
        e1 = hidden
        e2 = e1 + in_dim
        e3 = e2 + bott
        tails = full[:, e3:]
        loss = jnp.sum(tails.reshape(vp_size, qh, 128)[:, 0, 3])
        o_b_out = tails.reshape(vp_size, qh, 128)[:, :bq, 2].reshape(bott)
        return (loss, full[:, e1:e2].T, tails[:, 0], full[:, :e1], tails[:, 1], full[:, e2:e3], o_b_out, g_protos)

    by_rows = P('dp', None)
    by_cols = P(None, 'vp')
    replicated = P()
    head_specs = (replicated,) * 6
    in_specs = (by_rows, by_rows) + head_specs + (by_cols,) + head_specs + (by_cols,)
    out_specs = (replicated,) * 7 + (by_cols,)
    return jax.shard_map(local_step, mesh=mesh, in_specs=in_specs, out_specs=out_specs, check_vma=False)
```

```python
import functools

import jax
import jax.numpy as jnp
from jax import lax
from jax.experimental import pallas as pl
from jax.experimental.pallas import tpu as pltpu
from jax.sharding import PartitionSpec as P

ALL_CROPS = 10
GLOBAL_CROPS = 2
SINK_ITERS = 3
TEMP_STUDENT = 0.1
TEMP_TEACHER = 0.04
F32 = jnp.float32
BF16 = jnp.bfloat16
MESH = pl.DeviceIdType.MESH
LOG2E = 1.4426950408889634
CHUNK = 1024
OWN_CHUNK = 512


def gelu_slope(pre):
    cdf = 0.5 * (1.0 + lax.erf(pre * 0.7071067811865476))
    return cdf + pre * jnp.exp(-0.5 * pre * pre) * 0.3989422804014327


def mlp_forward(feats, w_in, b_in, w_mid, b_mid, w_out, b_out):
    pre_one = jnp.dot(feats, w_in, preferred_element_type=F32) + b_in.astype(F32)
    hid_one = jax.nn.gelu(pre_one, approximate=False).astype(BF16)
    pre_two = jnp.dot(hid_one, w_mid, preferred_element_type=F32) + b_mid.astype(F32)
    hid_two = jax.nn.gelu(pre_two, approximate=False).astype(BF16)
    proj = jnp.dot(hid_two, w_out, preferred_element_type=F32) + b_out.astype(F32)
    inv_norm = lax.rsqrt(jnp.sum(proj * proj, axis=-1, keepdims=True))
    unit = proj * inv_norm
    return unit.astype(BF16), proj, (pre_one, hid_one, pre_two, hid_two, unit, inv_norm)


def dot32(a, b):
    return jnp.dot(a, b, preferred_element_type=F32)


def main_kernel(cfg, t_ref, s_ref, pr_hbm, em_hbm, gemb_ref, stats_ref, bown_ref, loss_ref,
                em_v, us_v, e_v, lg_v, gl_v, col_s, col_r, col_a, b_v, srow_v, a_v, f_v, rowm_s, rowm_r, st_s, st_r,
                ld_sem, cs_sem, cr_sem, as_sem, ar_sem, rs_sem, rr_sem, ss_sem, sr_sem):
    n_dp, n_vp, n_proto, n_rows, scale = cfg
    me = lax.axis_index('dp')
    mv = lax.axis_index('vp')
    cb = CHUNK
    local = e_v.shape[1]
    own = local // n_dp
    n_chunk = local // cb
    ns = s_ref.shape[0]
    half = ns // ALL_CROPS
    c_exp = 10.0 * LOG2E
    lanes = cb // 128

    loads = []
    for c in range(n_chunk):
        loads.append((pltpu.make_async_copy(em_hbm.at[:, c * cb:(c + 1) * cb], em_v.at[:, c * cb:(c + 1) * cb], ld_sem.at[0, c]),
                      pltpu.make_async_copy(pr_hbm.at[:, c * cb:(c + 1) * cb], us_v.at[:, c * cb:(c + 1) * cb], ld_sem.at[1, c])))
    for c in range(n_chunk):
        loads[c][0].start()
    for c in range(n_chunk):
        loads[c][1].start()

    barrier = pltpu.get_barrier_semaphore()
    for j in range(1, n_dp):
        pl.semaphore_signal(barrier, inc=1, device_id={'dp': lax.rem(me + j, n_dp)}, device_id_type=MESH)
    for j in range(1, n_vp):
        pl.semaphore_signal(barrier, inc=1, device_id={'vp': lax.rem(mv + j, n_vp)}, device_id_type=MESH)
    pl.semaphore_wait(barrier, n_dp + n_vp - 2)

    def unit_block(ref, off):
        raw = ref[:, pl.ds(off, 128)].astype(F32)
        inv = lax.rsqrt(jnp.sum(raw * raw, axis=0, keepdims=True))
        return (raw * inv).astype(BF16)

    def wait_load(hbm, buf, which, c):
        pltpu.make_async_copy(hbm.at[:, pl.ds(c * cb, cb)], buf.at[:, pl.ds(c * cb, cb)], ld_sem.at[which, c]).wait()

    def teacher_body(c, carry):
        base = pl.multiple_of(c * cb, cb)
        wait_load(em_hbm, em_v, 0, c)
        for l in range(lanes):
            off = pl.multiple_of(base + l * 128, 128)
            em_v[:, pl.ds(off, 128)] = unit_block(em_v, off)
        e = jnp.exp(dot32(t_ref[...], em_v[:, pl.ds(base, cb)]) * (1.0 / TEMP_TEACHER))
        e_v[:, pl.ds(base, cb)] = e
        per = own // cb
        col_s[0, lax.div(c, per), :, pl.ds(pl.multiple_of(lax.rem(c, per) * cb, cb), cb)] = jnp.sum(e, axis=0, keepdims=True)
        return carry

    lax.fori_loop(0, n_chunk, teacher_body, 0)

    def start_cols(it):
        out = []
        for j in range(1, n_dp):
            peer = lax.rem(me + j, n_dp)
            cp = pltpu.make_async_remote_copy(
                src_ref=col_s.at[it, peer], dst_ref=col_r.at[it, me], send_sem=cs_sem.at[it, j], recv_sem=cr_sem.at[it, j],
                device_id={'dp': peer}, device_id_type=MESH)
            cp.start()
            out.append(cp)
        return out

    def finish_cols(it, copies):
        for cp in copies:
            cp.wait()
        tot = col_s[it, me]
        for j in range(1, n_dp):
            tot = tot + col_r[it, lax.rem(me + j, n_dp)]
        col_a[it, me] = tot
        out = []
        for j in range(1, n_dp):
            peer = lax.rem(me + j, n_dp)
            cp = pltpu.make_async_remote_copy(
                src_ref=col_a.at[it, me], dst_ref=col_a.at[it, me], send_sem=as_sem.at[it, j], recv_sem=ar_sem.at[it, j],
                device_id={'dp': peer}, device_id_type=MESH)
            cp.start()
            out.append(cp)
        for cp in out:
            cp.wait()

    def row_partial(it):
        per = own // cb
        for j in range(n_dp):
            inv = 1.0 / (col_a[it, j] * n_proto)
            for h in range(per):
                b_v[j * per + h] = inv[:, h * cb:(h + 1) * cb]

        def body(c, acc):
            for l in range(lanes):
                acc = acc + e_v[:, pl.ds(pl.multiple_of(c * cb + l * 128, 128), 128)] * b_v[c, :, l * 128:(l + 1) * 128]
            return acc
        acc = lax.fori_loop(0, n_chunk, body, jnp.zeros((e_v.shape[0], 128), F32))
        return jnp.sum(acc.T, axis=0, keepdims=True)

    def exchange_rows(it):
        out = []
        for j in range(1, n_vp):
            cp = pltpu.make_async_remote_copy(
                src_ref=rowm_s.at[it], dst_ref=rowm_r.at[it, mv], send_sem=rs_sem.at[it, j], recv_sem=rr_sem.at[it, j],
                device_id={'vp': lax.rem(mv + j, n_vp)}, device_id_type=MESH)
            cp.start()
            out.append(cp)
        for cp in out:
            cp.wait()
        rowm_r[it, mv] = rowm_s[it]
        tot = rowm_r[it, 0]
        for j in range(1, n_vp):
            tot = tot + rowm_r[it, j]
        return tot

    def col_partial(it):
        def body(c, carry):
            per = own // cb
            parts = []
            for l in range(lanes):
                x = e_v[:, pl.ds(pl.multiple_of(c * cb + l * 128, 128), 128)] * a_v[...]
                parts.append(jnp.sum(x, axis=0, keepdims=True))
            col_s[it, lax.div(c, per), :, pl.ds(pl.multiple_of(lax.rem(c, per) * cb, cb), cb)] = jnp.concatenate(parts, axis=1)
            return carry
        lax.fori_loop(0, n_chunk, body, 0)

    def to_column(row):
        return jnp.broadcast_to(row, (128, 128)).T

    copies = start_cols(0)

    srow_v[...] = jnp.zeros_like(srow_v)

    def student_body(c, carry):
        base = pl.multiple_of(c * cb, cb)
        wait_load(pr_hbm, us_v, 1, c)
        for l in range(lanes):
            off = pl.multiple_of(base + l * 128, 128)
            us_v[:, pl.ds(off, 128)] = unit_block(us_v, off)
        lg_v[...] = dot32(s_ref[...], us_v[:, pl.ds(base, cb)])
        for v in range(ALL_CROPS):
            rows = slice(v * half, (v + 1) * half)
            acc = srow_v[rows, :]
            for l in range(lanes):
                acc = acc + jnp.exp2(lg_v[rows, l * 128:(l + 1) * 128] * c_exp)
            srow_v[rows, :] = acc
        return carry

    lax.fori_loop(0, n_chunk, student_body, 0)

    finish_cols(0, copies)
    rowm_s[0, 0:1, :] = row_partial(0)
    n_sg = ns // 128
    for m in range(n_sg):
        rowm_s[0, m + 1:m + 2, :] = jnp.sum(srow_v[m * 128:(m + 1) * 128, :].T, axis=0, keepdims=True)
    tot = jnp.zeros((1, 128), F32)
    for j in range(n_dp):
        for l in range(own // 128):
            tot = tot + col_a[0, j, :, l * 128:(l + 1) * 128]
    rowm_s[0, n_sg + 1:n_sg + 2, :] = tot
    rowm_s[0, n_sg + 2:8, :] = jnp.zeros((8 - n_sg - 2, 128), F32)
    msg = exchange_rows(0)
    total = jnp.sum(msg[n_sg + 1:n_sg + 2, :], axis=1, keepdims=True)
    inv_total = 1.0 / total
    a_row = inv_total / ((msg[0:1, :] * (inv_total * total)) * n_rows)
    row_sum = msg[1:n_sg + 1, :]
    st_s[1:n_sg + 1, :] = row_sum
    st_s[n_sg + 1:8, :] = jnp.zeros((8 - n_sg - 1, 128), F32)
    for it in range(1, SINK_ITERS):
        a_v[...] = to_column(a_row)
        col_partial(it)
        finish_cols(it, start_cols(it))
        rowm_s[it, 0:1, :] = row_partial(it)
        rowm_s[it, 1:8, :] = jnp.zeros((7, 128), F32)
        msg = exchange_rows(it)
        a_row = 1.0 / (msg[0:1, :] * n_rows)
    a_fin = a_row * n_rows
    st_s[0:1, :] = a_fin
    st_copies = []
    for j in range(1, n_dp):
        cp = pltpu.make_async_remote_copy(
            src_ref=st_s, dst_ref=st_r.at[me], send_sem=ss_sem.at[j], recv_sem=sr_sem.at[j],
            device_id={'dp': lax.rem(me + j, n_dp)}, device_id_type=MESH)
        cp.start()
        st_copies.append(cp)
    k_g = scale / TEMP_STUDENT
    a_v[...] = to_column(a_fin * k_g)
    for m in range(n_sg):
        inv_rs = to_column(k_g / st_s[m + 1:m + 2, :])
        cnt0 = GLOBAL_CROPS - 1.0 if 2 * m < GLOBAL_CROPS else GLOBAL_CROPS * 1.0
        f_v[m * 128:(m + 1) * 128, :] = inv_rs * cnt0
    gemb_ref[...] = jnp.zeros_like(gemb_ref)

    def grad_body(c, carry):
        lx, ls0, ls1 = carry
        base = pl.multiple_of(c * cb, cb)
        u = us_v[:, pl.ds(base, cb)]
        lg_v[...] = dot32(s_ref[...], u)
        for l in range(lanes):
            cols = slice(l * 128, (l + 1) * 128)
            off = pl.multiple_of(base + l * 128, 128)
            b = b_v[c, :, cols]
            q0 = e_v[0:half, pl.ds(off, 128)] * a_v[0:half, :] * b
            q1 = e_v[half:2 * half, pl.ds(off, 128)] * a_v[half:2 * half, :] * b
            qs = q0 + q1
            ls0 = ls0 + q0
            ls1 = ls1 + q1
            for v in range(ALL_CROPS):
                rows = slice(v * half, (v + 1) * half)
                t = q1 if v == 0 else (q0 if v == 1 else qs)
                x = lg_v[rows, cols]
                gl_v[rows, cols] = (jnp.exp2(x * c_exp) * f_v[rows, :] - t).astype(BF16)
                lx = lx + t * x
        gemb_ref[...] += lax.dot_general(gl_v[...], u, (((1,), (1,)), ((), ())), preferred_element_type=F32)
        return lx, ls0, ls1

    z = jnp.zeros((half, 128), F32)
    lx, ls0, ls1 = lax.fori_loop(0, n_chunk, grad_body, (z, z, z))
    lpart = lx * (-1.0 / TEMP_STUDENT)
    for m in range(n_sg):
        lrs = to_column(jnp.log(st_s[m + 1:m + 2, :]))
        for h in range(2):
            v = 2 * m + h
            t = ls1 if v == 0 else (ls0 if v == 1 else ls0 + ls1)
            lpart = lpart + t * lrs[h * half:(h + 1) * half, :]
    loss_ref[...] = lpart * (1.0 / k_g * scale)
    bown_ref[...] = 1.0 / (col_a[SINK_ITERS - 1, me] * n_proto)
    for cp in st_copies:
        cp.wait()
    st_r[me] = st_s[...]
    stats_ref[...] = st_r[...]


def own_kernel(cfg, s_ref, st_ref, t_ref, stats_ref, b_ref, pr_ref, em_ref, out_ref, us_v, ut_v, lg_v, gl_v, a_v, f_v, gu_v):
    n_dp, scale = cfg
    own = out_ref.shape[1]
    cb = OWN_CHUNK
    ns = s_ref.shape[1]
    half = ns // ALL_CROPS
    n_sg = ns // 128
    k_g = scale / TEMP_STUDENT
    c_exp = 10.0 * LOG2E

    def unit_body(l, carry):
        off = pl.multiple_of(l * 128, 128)
        for src, dst in ((pr_ref, us_v), (em_ref, ut_v)):
            raw = src[:, pl.ds(off, 128)].astype(F32)
            inv = lax.rsqrt(jnp.sum(raw * raw, axis=0, keepdims=True))
            dst[:, pl.ds(off, 128)] = (raw * inv).astype(BF16)
        gu_v[:, pl.ds(off, 128)] = jnp.zeros((gu_v.shape[0], 128), F32)
        return carry

    lax.fori_loop(0, own // 128, unit_body, 0)

    def group_body(g, carry):
        stats = stats_ref[g]
        a_v[...] = jnp.broadcast_to(stats[0:1, :] * k_g, (128, 128)).T
        for m in range(n_sg):
            cnt0 = GLOBAL_CROPS - 1.0 if 2 * m < GLOBAL_CROPS else GLOBAL_CROPS * 1.0
            f_v[m * 128:(m + 1) * 128, :] = jnp.broadcast_to((k_g * cnt0) / stats[m + 1:m + 2, :], (128, 128)).T

        def chunk_body(c, carry2):
            base = pl.multiple_of(c * cb, cb)
            lg_v[...] = dot32(s_ref[g], us_v[:, pl.ds(base, cb)])
            e = jnp.exp(dot32(t_ref[g], ut_v[:, pl.ds(base, cb)]) * (1.0 / TEMP_TEACHER))
            b_all = b_ref[:, pl.ds(base, cb)]
            for l in range(cb // 128):
                cols = slice(l * 128, (l + 1) * 128)
                b = b_all[:, cols]
                q0 = e[0:half, cols] * a_v[0:half, :] * b
                q1 = e[half:2 * half, cols] * a_v[half:2 * half, :] * b
                qs = q0 + q1
                for v in range(ALL_CROPS):
                    rows = slice(v * half, (v + 1) * half)
                    t = q1 if v == 0 else (q0 if v == 1 else qs)
                    gl_v[rows, cols] = (jnp.exp2(lg_v[rows, cols] * c_exp) * f_v[rows, :] - t).astype(BF16)
            gu_v[:, pl.ds(base, cb)] += dot32(st_ref[g], gl_v[...])
            return carry2

        return lax.fori_loop(0, own // cb, chunk_body, carry)

    lax.fori_loop(0, n_dp, group_body, 0)

    def back_body(l, carry):
        off = pl.multiple_of(l * 128, 128)
        raw = pr_ref[:, pl.ds(off, 128)].astype(F32)
        inv = lax.rsqrt(jnp.sum(raw * raw, axis=0, keepdims=True))
        unit = raw * inv
        gu = gu_v[:, pl.ds(off, 128)]
        out_ref[:, pl.ds(off, 128)] = (gu - unit * jnp.sum(unit * gu, axis=0, keepdims=True)) * inv
        return carry

    lax.fori_loop(0, own // 128, back_body, 0)


def solution(mesh):
    vp_size = mesh.shape['vp']
    dp_size = mesh.shape['dp']

    def local_step(student_x, teacher_x, w_in, b_in, w_mid, b_mid, w_out, b_out, protos,
                   ema_w_in, ema_b_in, ema_w_mid, ema_b_mid, ema_w_out, ema_b_out, ema_protos):
        n_img = student_x.shape[0] // ALL_CROPS
        local_proto = protos.shape[1]
        n_proto = local_proto * vp_size
        n_rows = GLOBAL_CROPS * n_img * dp_size
        hidden = w_mid.shape[0]
        bott = w_out.shape[1]
        in_dim = w_in.shape[0]
        i_dp = lax.axis_index('dp')
        i_vp = lax.axis_index('vp')
        scale = 1.0 / (n_img * dp_size * GLOBAL_CROPS * (ALL_CROPS - 1))

        n_s = student_x.shape[0]
        n_t = teacher_x.shape[0]
        own = local_proto // dp_size
        student_x = student_x.reshape(n_img, ALL_CROPS, in_dim).swapaxes(0, 1).reshape(n_s, in_dim)
        teacher_x = teacher_x.reshape(n_img, GLOBAL_CROPS, in_dim).swapaxes(0, 1).reshape(n_t, in_dim)
        t_emb, t_proj, _ = mlp_forward(teacher_x, ema_w_in, ema_b_in, ema_w_mid, ema_b_mid, ema_w_out, ema_b_out)
        s_emb, s_proj, saved = mlp_forward(student_x, w_in, b_in, w_mid, b_mid, w_out, b_out)
        emb_all = lax.all_gather(jnp.concatenate([s_proj, t_proj], axis=0), 'dp', axis=0)
        emb_all = (emb_all * lax.rsqrt(jnp.sum(emb_all * emb_all, axis=-1, keepdims=True))).astype(BF16)

        sem = pltpu.SemaphoreType.DMA
        it = SINK_ITERS
        n_chunk = local_proto // CHUNK
        vm = pl.BlockSpec(memory_space=pltpu.VMEM)
        g_emb_part, stats, b_own, loss_part = pl.pallas_call(
            functools.partial(main_kernel, (dp_size, vp_size, float(n_proto), float(n_rows), scale)),
            out_shape=(jax.ShapeDtypeStruct((n_s, bott), F32), jax.ShapeDtypeStruct((dp_size, 8, 128), F32),
                       jax.ShapeDtypeStruct((1, own), F32), jax.ShapeDtypeStruct((n_img, 128), F32)),
            in_specs=[vm, vm, pl.BlockSpec(memory_space=pltpu.HBM), pl.BlockSpec(memory_space=pltpu.HBM)],
            out_specs=(vm, vm, vm, vm),
            scratch_shapes=[
                pltpu.VMEM((bott, local_proto), BF16), pltpu.VMEM((bott, local_proto), BF16),
                pltpu.VMEM((n_t, local_proto), F32), pltpu.VMEM((n_s, CHUNK), F32), pltpu.VMEM((n_s, CHUNK), BF16),
                pltpu.VMEM((it, dp_size, 1, own), F32), pltpu.VMEM((it, dp_size, 1, own), F32),
                pltpu.VMEM((it, dp_size, 1, own), F32), pltpu.VMEM((n_chunk, 1, CHUNK), F32),
                pltpu.VMEM((n_s, 128), F32), pltpu.VMEM((n_t, 128), F32), pltpu.VMEM((n_s, 128), F32),
                pltpu.VMEM((it, 8, 128), F32), pltpu.VMEM((it, vp_size, 8, 128), F32),
                pltpu.VMEM((8, 128), F32), pltpu.VMEM((dp_size, 8, 128), F32),
                sem((2, n_chunk)), sem((it, dp_size)), sem((it, dp_size)), sem((it, dp_size)), sem((it, dp_size)),
                sem((it, vp_size)), sem((it, vp_size)), sem((dp_size,)), sem((dp_size,))],
            compiler_params=pltpu.CompilerParams(collective_id=0, has_side_effects=True, vmem_limit_bytes=60 * 1024 * 1024),
            cost_estimate=pl.CostEstimate(flops=18 * 10 ** 9, bytes_accessed=20 * 10 ** 6, transcendentals=25 * 10 ** 6),
            name='sinkhorn_student',
        )(t_emb, s_emb, protos, ema_protos)
        g_emb = lax.psum(g_emb_part, 'vp')
        loss_part = jnp.sum(loss_part)

        c0 = i_dp * own
        s_all = emb_all[:, :n_s]
        gp_own = pl.pallas_call(
            functools.partial(own_kernel, (dp_size, scale)),
            out_shape=jax.ShapeDtypeStruct((bott, own), F32),
            in_specs=[vm] * 7, out_specs=vm,
            scratch_shapes=[pltpu.VMEM((bott, own), BF16), pltpu.VMEM((bott, own), BF16), pltpu.VMEM((n_s, OWN_CHUNK), F32),
                            pltpu.VMEM((n_s, OWN_CHUNK), BF16), pltpu.VMEM((n_t, 128), F32), pltpu.VMEM((n_s, 128), F32),
                            pltpu.VMEM((bott, own), F32)],
            compiler_params=pltpu.CompilerParams(vmem_limit_bytes=48 * 1024 * 1024),
            cost_estimate=pl.CostEstimate(flops=12 * 10 ** 9, bytes_accessed=12 * 10 ** 6, transcendentals=12 * 10 ** 6),
            name='own_columns',
        )(s_all, s_all.swapaxes(1, 2), emb_all[:, n_s:], stats, b_own,
          lax.dynamic_slice_in_dim(protos, c0, own, axis=1), lax.dynamic_slice_in_dim(ema_protos, c0, own, axis=1))
        g_protos = lax.all_gather(gp_own, 'dp', axis=1, tiled=True)

        pre_one, hid_one, pre_two, hid_two, unit, inv_norm = saved
        qh = hidden // vp_size
        h0 = i_vp * qh
        g_proj = (g_emb - unit * jnp.sum(unit * g_emb, axis=-1, keepdims=True)) * inv_norm
        g_proj_lo = g_proj.astype(BF16)
        g_hid_two = jnp.einsum('nb,hb->nh', g_proj_lo, w_out, preferred_element_type=F32)
        g_pre_two = g_hid_two * gelu_slope(pre_two)
        g_pre_two_lo = g_pre_two.astype(BF16)
        hid_two_q = lax.dynamic_slice_in_dim(hid_two, h0, qh, axis=1)
        hid_one_q = lax.dynamic_slice_in_dim(hid_one, h0, qh, axis=1)
        pre_one_q = lax.dynamic_slice_in_dim(pre_one, h0, qh, axis=1)
        w_mid_q = lax.dynamic_slice_in_dim(w_mid, h0, qh, axis=0)
        g_w_out_q = jnp.einsum('nh,nb->hb', hid_two_q, g_proj_lo, preferred_element_type=F32)
        g_w_mid_q = jnp.einsum('ng,nh->gh', hid_one_q, g_pre_two_lo, preferred_element_type=F32)
        g_hid_one_q = jnp.einsum('nh,gh->ng', g_pre_two_lo, w_mid_q, preferred_element_type=F32)
        g_pre_one_q = g_hid_one_q * gelu_slope(pre_one_q)
        g_w_in_q = jnp.einsum('nh,nf->hf', g_pre_one_q.astype(BF16), student_x, preferred_element_type=F32)
        bq = bott // vp_size
        gb_in = jnp.sum(g_pre_one_q, axis=0)
        gb_mid = lax.dynamic_slice_in_dim(jnp.sum(g_pre_two, axis=0), h0, qh, axis=0)
        gb_out = lax.dynamic_slice_in_dim(jnp.sum(g_proj, axis=0), i_vp * bq, bq, axis=0)
        tail = jnp.stack([gb_in, gb_mid, jnp.pad(gb_out, (0, qh - bq)),
                          jnp.pad(loss_part.reshape(1), (0, qh - 1))], axis=1)
        stack = jnp.concatenate([g_w_mid_q, g_w_in_q, g_w_out_q, jnp.pad(tail, ((0, 0), (0, 124)))], axis=1)
        part = lax.psum_scatter(stack, 'dp', scatter_dimension=0, tiled=True)
        full = lax.all_gather(part, ('vp', 'dp'), axis=0, tiled=True)
        e1 = hidden
        e2 = e1 + in_dim
        e3 = e2 + bott
        tails = full[:, e3:]
        loss = jnp.sum(tails.reshape(vp_size, qh, 128)[:, 0, 3])
        o_b_out = tails.reshape(vp_size, qh, 128)[:, :bq, 2].reshape(bott)
        return (loss, full[:, e1:e2].T, tails[:, 0], full[:, :e1], tails[:, 1], full[:, e2:e3], o_b_out, g_protos)

    by_rows = P('dp', None)
    by_cols = P(None, 'vp')
    replicated = P()
    head_specs = (replicated,) * 6
    in_specs = (by_rows, by_rows) + head_specs + (by_cols,) + head_specs + (by_cols,)
    out_specs = (replicated,) * 7 + (by_cols,)
    return jax.shard_map(local_step, mesh=mesh, in_specs=in_specs, out_specs=out_specs, check_vma=False)
```
